32 devices in a mesh: expert: 4 (over y, x), dp: 8 (over z, core).
Axes of the slice: x: 2, y: 2, z: 4, core: 2. Of those that a mesh axis runs over, the one named last changes fastest.
Arguments:
- x_new: bfloat16 [128, 4096], P('expert', 'dp'), may hold values from -6 to 6
- routes_new: int32 [128, 2], P('expert'), may hold values from 0 to 3, all different within a row; in each aligned block of 32 rows (0 to 31, 32 to 63, ...) at most 32 rows name the same one
- gates_new: float32 [128, 2], P('expert'), may hold values from 0.2 to 1
- w_gate: bfloat16 [4, 4096, 7168], P('expert', None, 'dp'), may hold values from -0.09375 to 0.09375
- w_up: bfloat16 [4, 4096, 7168], P('expert', None, 'dp'), may hold values from -0.09375 to 0.09375
- w_down: bfloat16 [4, 7168, 4096], P('expert', 'dp'), may hold values from -0.09375 to 0.09375
- grad_out: bfloat16 [256, 4096], P('expert', 'dp'), may hold values from -6 to 6
- routes_old: int32 [256, 2], P('expert'), may hold values from 0 to 3, all different within a row; in each aligned block of 64 rows (0 to 63, 64 to 127, ...) at most 64 rows name the same one
- gates_old: float32 [256, 2], P('expert'), may hold values from 0.2 to 1
- pre_gate: bfloat16 [4, 256, 7168], P('expert', None, 'dp'), may hold values from -8 to 8
- pre_up: bfloat16 [4, 256, 7168], P('expert', None, 'dp'), may hold values from -6 to 6
Outputs:
- mixed: bfloat16 [128, 4096], P('expert', 'dp')
- grad_down: bfloat16 [4, 7168, 4096], P('expert', 'dp')
- grad_gate: bfloat16 [4, 256, 7168], P('expert', None, 'dp')
- grad_up: bfloat16 [4, 256, 7168], P('expert', None, 'dp')
The draws below stay inside these ranges and needn't reach their ends.
Inputs may be any that keep to these rules, and one draw needn't show every extreme that they name: `routes_new`: in each group of 32 tokens each expert is named by at most 32 tokens, and by exactly 32 tokens in some group; the two experts of a token differ. `routes_old`: in each group of 64 tokens each expert is named by at most 64 tokens, and by exactly 64 tokens in some group; the two experts of a token differ.
All inputs are finite; a program needn't handle non-finite values.
Results may differ from the reference program's by a relative error of at most 0.0078.
Values may be sent and summed in bfloat16 or wider, within the bound.
A program may use at most 64 MiB of HBM per device.

```python
import math
import jax
import jax.numpy as jnp
import numpy as np
from jax import lax

D = 4096
FF = 7168
CAP_B = 32
CAP_A = 64
EXPERTS = 4
TOK_B = 32
TOK_A = 64
TOKENS_B = 128
TOKENS_A = 256


def raised(drawn, key, source, target, parts, factor):
    def block_of(dim):
        return (jnp.arange(drawn.shape[dim]) // (drawn.shape[dim] // parts)).reshape((-1,) + (1,) * (drawn.ndim - 1 - dim))

    near = jax.random.permutation(key, parts)[block_of(target)]
    other_side = (block_of(target) + parts // 2) % parts
    return jnp.where((block_of(source) == near) | (block_of(source) == other_side), factor * drawn, drawn)


def shard_levels(key, shape, cuts, least, largest):
    factor_of, own = 1.0, jax.random.fold_in(key, 6)
    for dim, parts in cuts:
        draws = jnp.exp(jax.random.uniform(jax.random.fold_in(own, dim), (parts,), jnp.float32, least / len(cuts), largest / len(cuts)))
        factor_of = factor_of * jnp.repeat(draws, shape[dim] // parts).reshape([-1 if axis == dim else 1 for axis in range(len(shape))])
    return factor_of


def assign_block(stream_key, own, number, rows, count, top, bound, skew):
    order = jax.random.permutation(stream_key, count)
    packed, common = portions_of(count, rows * top, bound, skew, True), portions_of(count, rows * top, bound, skew, False)
    places = jnp.arange(count)

    def named(sizes, offset_by):
        used = int((sizes > 0).sum())
        fixed = max(1, used // 4)
        passed = fixed + (places - fixed + offset_by * (used - fixed)) % max(1, count - fixed)
        return jnp.zeros((count,), jnp.int32).at[order[jnp.where(places < fixed, places, passed)]].set(jnp.asarray(sizes, jnp.int32))

    sizes = jnp.where(number % 4 == 0, named(packed, number // 4), named(common, number - number // 4 - 1))
    mixed = jax.random.permutation(jax.random.fold_in(own, 3), count)
    donor, receiver = mixed[0:count // 2 * 2:2], mixed[1:count // 2 * 2:2]
    margin = jnp.minimum(sizes[donor] - 1, bound - sizes[receiver]) // 2
    margin = jnp.where((donor == order[0]) | (receiver == order[0]) | (sizes[receiver] == 0), 0, jnp.maximum(margin, 0))
    passed = jax.random.randint(jax.random.fold_in(own, 4), (count // 2,), 0, 1 << 20) % (margin + 1)
    sizes = sizes.at[donor].add(-passed).at[receiver].add(passed)
    labels = jnp.searchsorted(jnp.cumsum(sizes), jnp.arange(rows * top), side="right").astype(jnp.int32)
    table = labels.reshape(top, rows).T
    table = table[jax.random.permutation(jax.random.fold_in(own, 1), rows)]
    offset_by = jax.random.randint(jax.random.fold_in(own, 2), (rows, 1), 0, top)
    return jnp.take_along_axis(table, (jnp.arange(top)[None, :] + offset_by) % top, axis=1)


def portions_of(number_of, total, reach, skew, full):
    weights = [(1 << 20) // math.isqrt(grade ** skew) + 1 for grade in range(1, number_of + 1)]
    largest = reach if full else min(reach, max(-(-total // number_of), total * weights[0] // sum(weights)))
    least = 1 if total - largest >= number_of - 1 else 0
    holding, spare = [largest] + [least] * (number_of - 1), total - largest - least * (number_of - 1)
    while spare > 0:
        movable = [i for i in range(1, number_of) if holding[i] < largest] or [i for i in range(1, number_of) if holding[i] < reach]
        mass, budget = sum([weights[i] for i in movable]), spare
        for i in movable:
            addition = min(reach - holding[i], max(1, budget * weights[i] // mass), spare)
            holding[i] = holding[i] + addition
            spare = spare - addition
    return np.array(holding)


def scatter_about(stream_key, extent, spread, reach, shards=(), held_as=jnp.bfloat16):
    level = shard_levels(stream_key, extent, shards, -0.22, 0.18) if shards else 1.0
    values = jax.random.normal(stream_key, extent, jnp.float32) * spread * level
    return jnp.minimum(jnp.maximum(values, -reach), reach).astype(held_as)


def gaussian_with(key, dims, spread, most, pieces, heavy, kind=jnp.bfloat16):
    result = spread * jax.random.normal(key, dims, jnp.float32)
    if pieces:
        result = result * shard_levels(key, dims, pieces, -0.22, 0.18)
    return jnp.clip(raised(result, jax.random.fold_in(key, 3), *heavy), -most, most).astype(kind)


def setup_inputs(seed: int = 0) -> dict:
    seeds = jax.random.split(jax.random.key(seed), 12)
    x_new = scatter_about(seeds[0], (TOKENS_B, D), 1.0, 6.0, ((0, 4), (1, 8)))
    routes_new_keys = jax.random.split(jax.random.fold_in(seeds[1], 1), TOKENS_B // TOK_B)
    routes_new_turns = jax.random.permutation(jax.random.fold_in(seeds[1], 3), TOKENS_B // TOK_B)
    routes_new = jax.vmap(lambda own, number: assign_block(jax.random.fold_in(seeds[1], 2), own, number, TOK_B, EXPERTS, 2, CAP_B, 2))(routes_new_keys, routes_new_turns).reshape((TOKENS_B, 2))
    gates_new = jnp.clip(0.2 + 0.8 * jax.random.uniform(seeds[2], (TOKENS_B, 2), jnp.float32) ** shard_levels(seeds[2], (TOKENS_B, 2), ((0, 4),), -0.2, 0.2), 0.2, 1.0)
    w_gate = scatter_about(seeds[3], (EXPERTS, D, FF), D ** -0.5, 0.09375, ((0, 4), (2, 8)))
    w_up = scatter_about(seeds[4], (EXPERTS, D, FF), D ** -0.5, 0.09375, ((0, 4), (2, 8)))
    w_down = gaussian_with(seeds[5], (EXPERTS, FF, D), FF ** -0.5, 0.09375, ((0, 4), (1, 8)), (1, 2, 8, 2.0))
    grad_out = scatter_about(seeds[6], (TOKENS_A, D), 1.0, 6.0, ((0, 4), (1, 8)))
    routes_old_keys = jax.random.split(jax.random.fold_in(seeds[7], 1), TOKENS_A // TOK_A)
    routes_old_turns = jax.random.permutation(jax.random.fold_in(seeds[7], 3), TOKENS_A // TOK_A)
    routes_old = jax.vmap(lambda own, number: assign_block(jax.random.fold_in(seeds[7], 2), own, number, TOK_A, EXPERTS, 2, CAP_A, 2))(routes_old_keys, routes_old_turns).reshape((TOKENS_A, 2))
    gates_old = jnp.clip(0.2 + 0.8 * jax.random.uniform(seeds[8], (TOKENS_A, 2), jnp.float32) ** shard_levels(seeds[8], (TOKENS_A, 2), ((0, 4),), -0.2, 0.2), 0.2, 1.0)
    pre_gate = scatter_about(seeds[9], (EXPERTS, EXPERTS * CAP_A, FF), 1.5, 8.0, ((0, 4), (2, 8)))
    pre_up = scatter_about(seeds[10], (EXPERTS, EXPERTS * CAP_A, FF), 1.0, 6.0, ((0, 4), (2, 8)))
    return {"x_new": x_new, "routes_new": routes_new, "gates_new": gates_new, "w_gate": w_gate, "w_up": w_up, "w_down": w_down, "grad_out": grad_out, "routes_old": routes_old, "gates_old": gates_old, "pre_gate": pre_gate, "pre_up": pre_up}


def slot_table(routes, capacity, experts):
    pairs = routes.reshape(-1)
    onehot = (pairs[:, None] == jnp.arange(experts, dtype=jnp.int32)[None, :]).astype(jnp.int32)
    before = jnp.cumsum(onehot, axis=0) - onehot
    slot = jnp.sum(before * onehot, axis=1)
    column = pairs * capacity + slot
    table = (jnp.arange(experts * capacity, dtype=jnp.int32)[:, None] == column[None, :]).astype(jnp.float32)
    return table.reshape(experts * capacity, routes.shape[0], 2)


def to_experts(buffers, capacity):
    groups = buffers.shape[0]
    width = buffers.shape[2]
    split = buffers.reshape(groups, groups, capacity, width)
    return jnp.transpose(split, (1, 0, 2, 3)).reshape(groups, groups * capacity, width)


def reference(x_new, routes_new, gates_new, w_gate, w_up, w_down, grad_out, routes_old, gates_old, pre_gate, pre_up):
    experts = EXPERTS
    tables = jax.vmap(lambda r: slot_table(r, CAP_B, experts))(routes_new.reshape(experts, TOK_B, 2))
    picks = jnp.sum(tables, axis=3)
    grouped = x_new.reshape(experts, TOK_B, D).astype(jnp.float32)
    buffers = jnp.einsum('sct,std->scd', picks, grouped, precision=lax.Precision.HIGHEST)
    expert_in = to_experts(buffers, CAP_B).astype(jnp.bfloat16)

    def forward(items):
        rows, gate_w, up_w, down_w = items
        gate_pre = jnp.dot(rows, gate_w, preferred_element_type=jnp.float32)
        up_pre = jnp.dot(rows, up_w, preferred_element_type=jnp.float32)
        hidden = (jax.nn.silu(gate_pre) * up_pre).astype(jnp.bfloat16)
        return jnp.dot(hidden, down_w, preferred_element_type=jnp.float32).astype(jnp.bfloat16)

    expert_out = lax.map(forward, (expert_in, w_gate, w_up, w_down))
    back = to_experts(expert_out, CAP_B).astype(jnp.float32)
    weighted = jnp.sum(tables * gates_new.reshape(experts, 1, TOK_B, 2), axis=3)
    mixed = jnp.einsum('sct,scd->std', weighted, back, precision=lax.Precision.HIGHEST)
    mixed = mixed.reshape(TOKENS_B, D).astype(jnp.bfloat16)

    tables_old = jax.vmap(lambda r: slot_table(r, CAP_A, experts))(routes_old.reshape(experts, TOK_A, 2))
    weighted_old = jnp.sum(tables_old * gates_old.reshape(experts, 1, TOK_A, 2), axis=3)
    grouped_old = grad_out.reshape(experts, TOK_A, D).astype(jnp.float32)
    cot_buffers = jnp.einsum('sct,std->scd', weighted_old, grouped_old, precision=lax.Precision.HIGHEST)
    cotangent = to_experts(cot_buffers.astype(jnp.bfloat16), CAP_A)

    def backward(items):
        rows, saved_gate, saved_up, down_w = items
        gate_pre = saved_gate.astype(jnp.float32)
        up_pre = saved_up.astype(jnp.float32)
        sigma = jax.nn.sigmoid(gate_pre)
        active = gate_pre * sigma
        hidden = (active * up_pre).astype(jnp.bfloat16)
        weight_grad = jnp.dot(hidden.T, rows, preferred_element_type=jnp.float32).astype(jnp.bfloat16)
        grad_hidden = jnp.dot(rows, down_w.T, preferred_element_type=jnp.float32)
        gate_grad = (grad_hidden * up_pre * sigma * (1.0 + gate_pre * (1.0 - sigma))).astype(jnp.bfloat16)
        up_grad = (grad_hidden * active).astype(jnp.bfloat16)
        return weight_grad, gate_grad, up_grad

    grad_down, grad_gate, grad_up = lax.map(backward, (cotangent, pre_gate, pre_up, w_down))
    return mixed, grad_down, grad_gate, grad_up
```

```python
import functools

import jax
import jax.numpy as jnp
from jax import lax
from jax.experimental import pallas as pl
from jax.experimental.pallas import tpu as pltpu
from jax.sharding import PartitionSpec as P

CAP_B = 32
CAP_A = 64


def slot_table(routes, capacity, experts):
    pairs = routes.reshape(-1)
    onehot = (pairs[:, None] == jnp.arange(experts, dtype=jnp.int32)[None, :]).astype(jnp.int32)
    before = jnp.cumsum(onehot, axis=0) - onehot
    slot = jnp.sum(before * onehot, axis=1)
    column = pairs * capacity + slot
    table = (jnp.arange(experts * capacity, dtype=jnp.int32)[:, None] == column[None, :]).astype(
        jnp.float32
    )
    return table.reshape(experts * capacity, routes.shape[0], 2)


def per_device(
    x_new,
    routes_new,
    gates_new,
    w_gate,
    w_up,
    w_down,
    grad_out,
    routes_old,
    gates_old,
    pre_gate,
    pre_up,
):
    experts = lax.axis_size("expert")
    slice_width = x_new.shape[1]
    gate_weight = w_gate[0]
    up_weight = w_up[0]
    down_weight = w_down[0]
    rows_new = experts * CAP_B
    rows_old = experts * CAP_A
    table_new = slot_table(routes_new, CAP_B, experts)
    picks = jnp.sum(table_new, axis=2).astype(jnp.bfloat16)
    outgoing = jnp.dot(picks, x_new, preferred_element_type=jnp.float32).astype(jnp.bfloat16)
    arrived = lax.all_to_all(
        outgoing.reshape(experts, CAP_B, slice_width),
        "expert",
        split_axis=0,
        concat_axis=0,
        tiled=True,
    )
    arrived = arrived.reshape(rows_new, slice_width)
    piece = lax.all_gather(arrived, "dp", axis=1, tiled=True)
    gate_pre = jnp.dot(piece, gate_weight, preferred_element_type=jnp.float32)
    up_pre = jnp.dot(piece, up_weight, preferred_element_type=jnp.float32)
    hidden = (jax.nn.silu(gate_pre) * up_pre).astype(jnp.bfloat16)
    partial_value = jnp.dot(hidden, down_weight, preferred_element_type=jnp.float32)
    result = lax.psum_scatter(partial_value, "dp", scatter_dimension=1, tiled=True).astype(
        jnp.bfloat16
    )
    returned = lax.all_to_all(
        result.reshape(experts, CAP_B, slice_width),
        "expert",
        split_axis=0,
        concat_axis=0,
        tiled=True,
    )
    returned = returned.reshape(rows_new, slice_width)
    weights_new = jnp.sum(table_new * gates_new[None, :, :], axis=2)
    mixed = jnp.dot(
        weights_new.T, returned.astype(jnp.float32), precision=lax.Precision.HIGHEST
    ).astype(jnp.bfloat16)
    table_old = slot_table(routes_old, CAP_A, experts)
    weights_old = jnp.sum(table_old * gates_old[None, :, :], axis=2)
    cotangent = jnp.dot(
        weights_old, grad_out.astype(jnp.float32), precision=lax.Precision.HIGHEST
    ).astype(jnp.bfloat16)
    landed = lax.all_to_all(
        cotangent.reshape(experts, CAP_A, slice_width),
        "expert",
        split_axis=0,
        concat_axis=0,
        tiled=True,
    )
    landed = landed.reshape(rows_old, slice_width)
    saved_gate = pre_gate[0].astype(jnp.float32)
    saved_up = pre_up[0].astype(jnp.float32)
    sigma = jax.nn.sigmoid(saved_gate)
    active = saved_gate * sigma
    hidden_old = (active * saved_up).astype(jnp.bfloat16)
    piece = lax.all_gather(landed, "dp", axis=1, tiled=True)
    grad_hidden = lax.dot_general(
        piece, down_weight, (((1,), (1,)), ((), ())), preferred_element_type=jnp.float32
    )
    block = lax.dot_general(
        hidden_old, piece, (((0,), (0,)), ((), ())), preferred_element_type=jnp.float32
    )
    weight_grad = block
    grad_hidden, weight_grad = (grad_hidden, weight_grad)
    gate_grad = (grad_hidden * saved_up * sigma * (1.0 + saved_gate * (1.0 - sigma))).astype(
        jnp.bfloat16
    )
    up_grad = (grad_hidden * active).astype(jnp.bfloat16)
    return (mixed, weight_grad.astype(jnp.bfloat16)[None], gate_grad[None], up_grad[None])


MESH = pl.DeviceIdType.MESH
F32 = jnp.float32
BF16 = jnp.bfloat16


def exchange_kernel(
    ne,
    nz,
    x_hbm,
    g_hbm,
    ro_hbm,
    go_hbm,
    rn_hbm,
    gn_hbm,
    pg_hbm,
    pu_hbm,
    wg_hbm,
    wu_hbm,
    wd_hbm,
    mixed_ref,
    out_ref,
    cot_ref,
    wd,
    factor,
    active,
    xg,
    gg,
    ro_all,
    go_all,
    rn_all,
    gn_all,
    pg_ref,
    pu_ref,
    wg,
    wu,
    hsum,
    usum,
    hnew,
    hid_ref,
    pick_ref,
    gate_rows,
    psend,
    precv,
    pown,
    rsend,
    rrecv,
    zsend,
    zrecv,
    wsem,
    lsem,
    ms,
    mr,
    x1s,
    x1r,
    x2s,
    x2r,
    x3s,
    x3r,
    g1s,
    g1r,
    g2s,
    g2r,
    g3s,
    g3r,
    ps,
    pr,
    rs,
    rr,
    zs,
    zr,
):
    e = lax.axis_index("expert")
    d = lax.axis_index("dp")
    z = d // 2
    c = d % 2
    other = z * 2 + 1 - c
    tb, width = x_hbm.shape
    ta = g_hbm.shape[0]
    hidden = wg.shape[2]

    inner = jnp.minimum(z, nz - 1 - z)
    outward = jnp.where(z < nz - 1 - z, 1, -1)

    def near(j):
        beside = jnp.where(j % 2 == 1, -((j + 1) // 2), j // 2)
        return z + jnp.where(j <= 2 * inner, beside, outward * (j - inner))

    def back_by(j):
        return lax.rem(z + nz - near(j), nz)

    def rows(i, size):
        return pl.ds(pl.multiple_of(i * size, size), size)

    def peer(k):
        return lax.rem(e + k, ne)

    def remote(src, dst, ssem, rsem, to):
        return pltpu.make_async_remote_copy(
            src_ref=src, dst_ref=dst, send_sem=ssem, recv_sem=rsem, device_id=to, device_id_type=MESH
        )

    def block(buf, slot, size):
        return buf.at[slot, rows(e, size)]

    def first(buf, size, s, r, k):
        to = lax.rem(z + k, nz) * 2 + c
        return remote(block(buf, d, size), block(buf, d, size), s.at[k - 1], r.at[k - 1], (e, to))

    col, row = e % 2, e // 2
    sides = (row * 2 + 1 - col, (1 - row) * 2 + col)
    corner = (1 - row) * 2 + 1 - col

    def second(buf, size, s, r, j, k):
        place = block(buf, near(j) * 2 + c, size)
        i = j * 4 + k
        return remote(place, place, s.at[i], r.at[i], (sides[k], d))

    def second_in(buf, size, s, r, j, k):
        place = buf.at[near(j) * 2 + c, rows(sides[k], size)]
        return remote(place, place, s.at[j * 4 + k], r.at[j * 4 + k], (sides[k], d))

    def half(buf, who, size, j, k):
        start = pl.multiple_of(who * size + k * (size // 2), size // 2)
        return buf.at[near(j) * 2 + c, pl.ds(start, size // 2)]

    def relay(buf, size, s, r, j, k):
        place = half(buf, sides[k], size, j, k)
        i = j * 4 + 2 + k
        return remote(place, place, s.at[i], r.at[i], (sides[1 - k], d))

    def relay_in(buf, size, s, r, j, k):
        place = half(buf, corner, size, j, k)
        i = j * 4 + 2 + k
        return remote(place, place, s.at[i], r.at[i], (sides[1 - k], d))

    def pass_on(buf, size, s, r, j):
        for k in range(2):
            second_in(buf, size, s, r, j, k).wait_recv()
            relay(buf, size, s, r, j, k).start()

    def third(buf, s, r, j):
        slot = near(j) * 2 + c
        return remote(buf.at[slot], buf.at[slot], s.at[j], r.at[j], (e, other))

    def third_in(buf, s, r, j):
        slot = near(j) * 2 + 1 - c
        return remote(buf.at[slot], buf.at[slot], s.at[j], r.at[j], (e, other))

    def first_in(buf, size, s, r, j):
        slot = near(j) * 2 + c
        place = block(buf, slot, size)
        i = back_by(j) - 1
        return remote(place, place, s.at[i], r.at[i], (e, slot))

    def order(i):
        return near(i % nz) * 2 + jnp.where(i < nz, c, 1 - c)

    def load_in(slot):
        part = rows(slot, width)
        return (
            pltpu.make_async_copy(wg_hbm.at[0, part], wg.at[slot], wsem.at[0, slot]),
            pltpu.make_async_copy(wu_hbm.at[0, part], wu.at[slot], wsem.at[1, slot]),
        )

    def load_down(slot):
        return pltpu.make_async_copy(wd_hbm.at[0, :, rows(slot, width)], wd.at[slot], wsem.at[2, slot])

    def from_own(i):
        return lax.rem(d + i, 2 * nz)

    own_x = pltpu.make_async_copy(x_hbm, block(xg, d, tb), lsem.at[0])
    own_g = pltpu.make_async_copy(g_hbm, block(gg, d, ta), lsem.at[1])
    own_a = pltpu.make_async_copy(pg_hbm, pg_ref, lsem.at[2])
    own_b = pltpu.make_async_copy(pu_hbm, pu_ref, lsem.at[3])
    notes = ((ro_hbm, ro_all), (go_hbm, go_all), (rn_hbm, rn_all), (gn_hbm, gn_all))
    own_notes = [
        pltpu.make_async_copy(own, there.at[e], lsem.at[4 + n]) for n, (own, there) in enumerate(notes)
    ]
    own_x.start()
    own_g.start()
    for load in own_notes:
        load.start()

    barrier = pltpu.get_barrier_semaphore()
    friends = [(peer(k), d) for k in range(1, ne)]
    friends += [(e, lax.rem(z + k, nz) * 2 + c) for k in range(1, nz)]
    friends += [(e, other)]
    for to in friends:
        pl.semaphore_signal(barrier, inc=1, device_id=to, device_id_type=MESH)
    own_a.start()
    own_b.start()

    @pl.loop(0, 2 * nz)
    def _(i):
        for load in load_in(from_own(i)):
            load.start()

    @pl.loop(0, 2 * nz)
    def _(i):
        load_down(from_own(i)).start()

    own_x.wait()
    own_g.wait()
    for load in own_notes:
        load.wait()
    pl.semaphore_wait(barrier, len(friends))

    def note_to(n, k):
        there = notes[n][1].at[e]
        i = n * (ne - 1) + k - 1
        return remote(there, there, ms.at[i], mr.at[i], (peer(k), d))

    def note_in(n, k):
        place = notes[n][1].at[lax.rem(e + ne - k, ne)]
        i = n * (ne - 1) + k - 1
        return remote(place, place, ms.at[i], mr.at[i], (peer(k), d))

    for j in range(1, nz):
        first(xg, tb, x1s, x1r, nz - back_by(j)).start()
    for k in range(2):
        second(xg, tb, x2s, x2r, 0, k).start()
    for n in range(4):
        for k in range(1, ne):
            note_to(n, k).start()
    for k in range(2):
        second(gg, ta, g2s, g2r, 0, k).start()

    step = 32
    wide = 128
    own_a.wait()
    own_b.wait()

    @pl.loop(0, pg_ref.shape[0] // wide)
    def _(i):
        r = rows(i, wide)
        v = pg_ref[r].astype(F32)
        u = pu_ref[r].astype(F32)
        s = jax.nn.sigmoid(v)
        a = v * s
        active[r] = a
        factor[r] = u * s * (1.0 + v * (1.0 - s))
        hid_ref[:, r] = (a * u).T.astype(BF16)

    pass_on(xg, tb, x2s, x2r, 0)
    for j in range(1, nz):
        first(gg, ta, g1s, g1r, nz - back_by(j)).start()
    for j in range(1, nz):
        first_in(xg, tb, x1s, x1r, j).wait_recv()
        for k in range(2):
            second(xg, tb, x2s, x2r, j, k).start()

    for n in range(4):
        for k in range(1, ne):
            note_in(n, k).wait_recv()

    def joined(there):
        return jnp.concatenate([there[g] for g in range(ne)], axis=1)

    mine = e
    routes_a, routes_b = joined(ro_all), joined(rn_all)
    all_a, all_b = joined(go_all), joined(gn_all)
    hit0 = routes_a[0:1] == mine
    hit1 = routes_a[1:2] == mine
    gates_a = jnp.where(hit0, all_a[0:1], 0.0) + jnp.where(hit1, all_a[1:2], 0.0)
    named = jnp.where(hit0 | hit1, 1.0, 0.0)
    na = named.shape[1]
    ri = lax.broadcasted_iota(jnp.int32, (na, na), 0)
    ci = lax.broadcasted_iota(jnp.int32, (na, na), 1)
    base = ci // ta * ta
    earlier = jnp.where((ri < ci) & (ri >= base), 1.0, 0.0).astype(BF16)
    before = jnp.dot(
        jnp.broadcast_to(named, (16, na)).astype(BF16), earlier, preferred_element_type=F32
    )[0:1]
    target = jnp.where(named > 0.5, before, -1.0 * na)
    chosen = (ri - base).astype(F32) == target
    pick_ref[...] = jnp.where(chosen, 1.0, 0.0).astype(BF16)
    gate_rows[...] = jnp.broadcast_to(
        jnp.sum(jnp.where(chosen, gates_a, 0.0), axis=1, keepdims=True), gate_rows.shape
    )
    nb = ne * tb
    gates_b = jnp.where(routes_b[0:1] == mine, all_b[0:1], 0.0) + jnp.where(
        routes_b[1:2] == mine, all_b[1:2], 0.0
    )
    rb = lax.broadcasted_iota(jnp.int32, (nb, nb), 0)
    cb = lax.broadcasted_iota(jnp.int32, (nb, nb), 1)
    row_b = jnp.sum(jnp.where(rb == cb, gates_b, 0.0), axis=1, keepdims=True)
    hsum[...] = jnp.zeros_like(hsum)
    usum[...] = jnp.zeros_like(usum)

    for j in range(1, nz):
        pass_on(xg, tb, x2s, x2r, j)
        if j == nz - 2:
            pass_on(gg, ta, g2s, g2r, 0)

    def project(*steps):
        slots = [order(i) for i in steps]
        for slot in slots:
            for load in load_in(slot):
                load.wait()
        for total, w in ((hsum, wg), (usum, wu)):
            parts = [jnp.dot(xg[slot], w[slot], preferred_element_type=F32) for slot in slots]
            total[...] += sum(parts[1:], parts[0])

    def collect(i):
        for k in range(2):
            relay_in(xg, tb, x2s, x2r, i, k).wait_recv()
        third(xg, x3s, x3r, i).start()

    def spread_plane(j):
        first_in(gg, ta, g1s, g1r, j).wait_recv()
        for k in range(2):
            second(gg, ta, g2s, g2r, j, k).start()

    def arrive(j):
        for k in range(2):
            relay_in(gg, ta, g2s, g2r, j, k).wait_recv()
        third(gg, g3s, g3r, j).start()

    spread_plane(1)

    collect(0)
    collect(1)
    project(0, 1)
    for j in range(2, nz - 1):
        spread_plane(j)

    @pl.loop(2, nz)
    def _(i):
        collect(i)

        @pl.when(i == 2)
        def _():
            arrive(0)

        third_in(xg, x3s, x3r, i - 2).wait_recv()
        project(i, i - 2 + nz)

        @pl.when(i == 2)
        def _():
            spread_plane(nz - 1)
            pass_on(gg, ta, g2s, g2r, 1)

    third_in(xg, x3s, x3r, nz - 2).wait_recv()
    third_in(xg, x3s, x3r, nz - 1).wait_recv()
    project(2 * nz - 2, 2 * nz - 1)

    for j in range(2, nz - 1):
        pass_on(gg, ta, g2s, g2r, j)

    @pl.loop(0, nb // step)
    def _(i):
        r = rows(i, step)
        v = hsum[r]
        hnew[r] = (v * jax.nn.sigmoid(v) * usum[r]).astype(BF16)

    def to_other(j):
        return remote(psend.at[j], precv.at[j], ps.at[j], pr.at[j], (e, other))

    def to_group(j, k):
        i = j * (ne - 1) + k - 1
        return remote(
            rsend.at[j, rows(peer(k), tb)], rrecv.at[i], rs.at[i], rr.at[i], (peer(k), d)
        )

    def pair_sum(j):
        to_other(j).wait_recv()
        total = pown[j] + precv[j].astype(F32)
        pown[j] = total
        rsend[j] = total.astype(BF16)
        for k in range(1, ne):
            to_group(j, k).start()

    group = 2 if nz % 2 == 0 else 1

    @pl.loop(0, nz // group)
    def _(i):
        planes = [nz - 1 - i * group - n for n in range(group)]
        for j in planes:
            for k in range(2):
                load_down(near(j) * 2 + k).wait()
        for j in planes:
            out = jnp.dot(hnew[...], wd[near(j) * 2 + 1 - c], preferred_element_type=F32)
            psend[j] = (out * row_b).astype(BF16)
            out = jnp.dot(hnew[...], wd[near(j) * 2 + c], preferred_element_type=F32)
            pown[j] = out * row_b
        for j in planes:
            to_other(j).start()

        @pl.when(i == 0)
        def _():
            arrive(1)
            pass_on(gg, ta, g2s, g2r, nz - 1)

    def to_depth(j):
        to = lax.rem(z + nz - j, nz) * 2 + c
        return remote(zsend.at[j - 1], zrecv.at[j - 1], zs.at[j - 1], zr.at[j - 1], (e, to))

    def group_sum(j):
        for k in range(1, ne):
            to_group(j, k).wait_recv()
        total = pown[j, rows(e, tb)]
        for k in range(1, ne):
            total = total + rrecv[j * (ne - 1) + k - 1].astype(F32)
        return total

    def send_depth(j):
        i = back_by(j)
        zsend[i - 1] = group_sum(j).astype(BF16)
        to_depth(i).start()

    def spread(j):
        for n in range(2):
            moved = jnp.dot(pick_ref[...], gg[near(j) * 2 + n], preferred_element_type=F32)
            for m in range(width // wide):
                start = near(j) * 2 * width + n * width + m * wide
                cot_ref[:, pl.ds(pl.multiple_of(start, wide), wide)] = (
                    moved[:, m * wide : (m + 1) * wide] * gate_rows[...]
                ).astype(BF16)

    def outer(j):
        cols = rows(near(j), 2 * width)
        size = hidden // 2
        for n in range(2):
            part = pl.ds(n * size, size)
            out_ref[part, cols] = jnp.dot(
                hid_ref[part], cot_ref[:, cols], preferred_element_type=F32
            ).astype(BF16)

    third_in(gg, g3s, g3r, 0).wait_recv()
    spread(0)
    for j in range(nz - 1, nz // 2 - 1, -1):
        pair_sum(j)
    @pl.loop(1, nz)
    def _(i):
        third_in(gg, g3s, g3r, i).wait_recv()
        outer(i - 1)
        spread(i)
        @pl.when(i == 1)
        def _():
            for j in range(nz // 2 - 1, -1, -1):
                pair_sum(j)

        @pl.when(i + 1 < nz)
        def _():
            arrive(i + 1)

        @pl.when(i == nz - 2)
        def _():
            send_depth(nz - 1)

    for j in range(nz - 2, 0, -1):
        send_depth(j)
    outer(nz - 1)
    kept = group_sum(0)

    for j in range(1, nz):
        to_depth(j).wait_recv()
        kept = kept + zrecv[j - 1].astype(F32)
    mixed_ref[...] = kept.astype(BF16)

    for k in range(1, nz):
        first(xg, tb, x1s, x1r, k).wait_send()
        first(gg, ta, g1s, g1r, k).wait_send()
        to_depth(k).wait_send()
    for n in range(4):
        for k in range(1, ne):
            note_to(n, k).wait_send()
    for j in range(nz):
        for k in range(1, ne):
            to_group(j, k).wait_send()
        for k in range(2):
            second(xg, tb, x2s, x2r, j, k).wait_send()
            second(gg, ta, g2s, g2r, j, k).wait_send()
            relay(xg, tb, x2s, x2r, j, k).wait_send()
            relay(gg, ta, g2s, g2r, j, k).wait_send()
        third(xg, x3s, x3r, j).wait_send()
        third(gg, g3s, g3r, j).wait_send()
        to_other(j).wait_send()


def write_kernel(
    pieces,
    m_ref,
    w_ref,
    cot_ref,
    wd,
    factor,
    active,
    m_out,
    g_out,
    u_out,
    w_out,
    grad_ref,
    g_ref,
    u_ref,
    sem,
    gsem,
):
    size = w_ref.shape[0] // pieces
    pairs = [(w_ref.at[pl.ds(n * size, size)], w_out.at[pl.ds(n * size, size)]) for n in range(pieces)]
    pairs += [(m_ref, m_out)]
    copies = [pltpu.make_async_copy(src, dst, sem.at[n]) for n, (src, dst) in enumerate(pairs)]
    for copy in copies:
        copy.start()
    half = wd.shape[1] // 2
    width = wd.shape[2]
    for m in range(2):
        part = pl.ds(m * half, half)
        parts = [
            lax.dot_general(
                wd[i, part],
                cot_ref[:, pl.ds(i * width, width)],
                (((1,), (1,)), ((), ())),
                preferred_element_type=F32,
            )
            for i in range(wd.shape[0])
        ]
        grad_ref[part] = sum(parts[1:], parts[0])
    wide = 128
    for i in range(grad_ref.shape[0] // wide):
        r = pl.ds(i * wide, wide)
        grad = grad_ref[r].T
        g_ref[:, r] = (grad * factor[:, r]).astype(BF16)
        u_ref[:, r] = (grad * active[:, r]).astype(BF16)
    last = [pltpu.make_async_copy(g_ref, g_out, gsem.at[0]), pltpu.make_async_copy(u_ref, u_out, gsem.at[1])]
    for copy in last:
        copy.start()
    for copy in copies + last:
        copy.wait()


def per_device_fused(
    x_new,
    routes_new,
    gates_new,
    w_gate,
    w_up,
    w_down,
    grad_out,
    routes_old,
    gates_old,
    pre_gate,
    pre_up,
):
    ne = lax.axis_size("expert")
    ndp = lax.axis_size("dp")
    nz = ndp // 2
    tb, width = x_new.shape
    ta = grad_out.shape[0]
    hidden = w_gate.shape[2]
    na, nb = ne * ta, ne * tb
    vmem = pl.BlockSpec(memory_space=pltpu.VMEM)
    hbm = pl.BlockSpec(memory_space=pltpu.HBM)

    def pair(count):
        return [pltpu.SemaphoreType.DMA((count,)), pltpu.SemaphoreType.DMA((count,))]

    gather_sems = pair(nz - 1) + pair(nz * 4) + pair(nz)
    mixed, weight_grad, *state = pl.pallas_call(
        functools.partial(exchange_kernel, ne, nz),
        out_shape=(
            jax.ShapeDtypeStruct((tb, width), BF16),
            jax.ShapeDtypeStruct((hidden, ndp * width), BF16),
            jax.ShapeDtypeStruct((na, ndp * width), BF16),
            jax.ShapeDtypeStruct((ndp, hidden, width), BF16),
            jax.ShapeDtypeStruct((na, hidden), F32),
            jax.ShapeDtypeStruct((na, hidden), F32),
        ),
        in_specs=[hbm] * 11,
        out_specs=(vmem,) * 6,
        scratch_shapes=[
            pltpu.VMEM((ndp, nb, width), BF16),
            pltpu.VMEM((ndp, na, width), BF16),
            pltpu.VMEM((ne, 2, ta), jnp.int32),
            pltpu.VMEM((ne, 2, ta), F32),
            pltpu.VMEM((ne, 2, tb), jnp.int32),
            pltpu.VMEM((ne, 2, tb), F32),
            pltpu.VMEM((na, hidden), BF16),
            pltpu.VMEM((na, hidden), BF16),
            pltpu.VMEM((ndp, width, hidden), BF16),
            pltpu.VMEM((ndp, width, hidden), BF16),
            pltpu.VMEM((nb, hidden), F32),
            pltpu.VMEM((nb, hidden), F32),
            pltpu.VMEM((nb, hidden), BF16),
            pltpu.VMEM((hidden, na), BF16),
            pltpu.VMEM((na, na), BF16),
            pltpu.VMEM((na, 128), F32),
            pltpu.VMEM((nz, nb, width), BF16),
            pltpu.VMEM((nz, nb, width), BF16),
            pltpu.VMEM((nz, nb, width), F32),
            pltpu.VMEM((nz, nb, width), BF16),
            pltpu.VMEM((nz * (ne - 1), tb, width), BF16),
            pltpu.VMEM((nz - 1, tb, width), BF16),
            pltpu.VMEM((nz - 1, tb, width), BF16),
            pltpu.SemaphoreType.DMA((3, ndp)),
            pltpu.SemaphoreType.DMA((8,)),
        ]
        + pair(4 * (ne - 1))
        + gather_sems
        + gather_sems
        + pair(nz)
        + pair(nz * (ne - 1))
        + pair(nz - 1),
        compiler_params=pltpu.CompilerParams(
            collective_id=0, has_side_effects=True, vmem_limit_bytes=34 * 1024 * 1024
        ),
        name="exchange",
    )(
        *(
            pltpu.with_memory_space_constraint(value, pltpu.HBM)
            for value in (
                x_new,
                grad_out,
                routes_old.T,
                gates_old.T,
                routes_new.T,
                gates_new.T,
                pre_gate[0],
                pre_up[0],
                w_gate,
                w_up,
                w_down,
            )
        )
    )
    parts = next(n for n in (8, 7, 4, 2, 1) if hidden % (n * 16) == 0)
    mixed, gate_grad, up_grad, weight_grad = pl.pallas_call(
        functools.partial(write_kernel, parts),
        out_shape=(
            jax.ShapeDtypeStruct((tb, width), BF16),
            jax.ShapeDtypeStruct((na, hidden), BF16),
            jax.ShapeDtypeStruct((na, hidden), BF16),
            jax.ShapeDtypeStruct((hidden, ndp * width), BF16),
        ),
        in_specs=[vmem] * 6,
        out_specs=(hbm,) * 4,
        scratch_shapes=[
            pltpu.VMEM((hidden, na), F32),
            pltpu.VMEM((na, hidden), BF16),
            pltpu.VMEM((na, hidden), BF16),
            pltpu.SemaphoreType.DMA((parts + 1,)),
            pltpu.SemaphoreType.DMA((2,)),
        ],
        compiler_params=pltpu.CompilerParams(vmem_limit_bytes=8 * 1024 * 1024),
        name="write",
    )(mixed, weight_grad, *state)
    return (mixed, weight_grad[None], gate_grad[None], up_grad[None])


def pick_body(mesh):
    ne, ndp = mesh.shape["expert"], mesh.shape["dp"]

    def body(*args):
        x_new, w_gate = args[0], args[3]
        whole_tiles = x_new.shape[1] % 128 == 0 and w_gate.shape[2] % 128 == 0
        full_slots = x_new.shape[0] == CAP_B and args[6].shape[0] == CAP_A
        if ndp % 2 == 0 and ndp > 2 and ne == 4 and whole_tiles and full_slots:
            return per_device_fused(*args)
        return per_device(*args)

    return body


def solution(mesh):
    body = pick_body(mesh)
    placed = (
        P("expert", "dp"),
        P("expert", None),
        P("expert", None),
        P("expert", None, "dp"),
        P("expert", None, "dp"),
        P("expert", "dp", None),
        P("expert", "dp"),
        P("expert", None),
        P("expert", None),
        P("expert", None, "dp"),
        P("expert", None, "dp"),
    )
    return jax.shard_map(
        body,
        mesh=mesh,
        in_specs=placed,
        out_specs=(
            P("expert", "dp"),
            P("expert", "dp", None),
            P("expert", None, "dp"),
            P("expert", None, "dp"),
        ),
        check_vma=False,
    )
```
